32 devices in a mesh: grp: 4 (over y, core), ep: 8 (over z, x).
Axes of the slice: x: 2, y: 2, z: 4, core: 2. Of those that a mesh axis runs over, the one named last changes fastest.
Arguments:
- d_out: bfloat16 [4096, 2048], P(('grp', 'ep')), may hold values from -12 to 12
- routes: int32 [4096, 2], P(('grp', 'ep')), may hold values from 0 to 7, all different within a row; in each aligned block of 128 rows (0 to 127, 128 to 255, ...) at most 48 rows name the same one
- combine: float32 [4096, 2], P(('grp', 'ep')), may hold values from 0.05 to 1
- live_tokens: int32 [32], P(('grp', 'ep')), may hold values from 1 to 128, as said below
- hidden: bfloat16 [1536, 57344], P('grp', 'ep'), may hold values from -6 to 6
Outputs:
- expert_grad: float32 [2048, 57344], P('grp', 'ep')
The draws below stay inside these ranges and needn't reach their ends.
Inputs may be any that keep to these rules, and one draw needn't show every extreme that they name: `routes`: the two experts of a token differ. Among the 128 rows of one device no expert is named by more than 48 rows, and on some devices one expert is named by exactly 48 rows. `live_tokens`: the live tokens of a device are its first ones; on the last device all 128 are live.
All inputs are finite; a program needn't handle non-finite values.
Results may differ from the reference program's by a relative error of at most 0.0029.
Values may be sent and summed in bfloat16 or wider, within the bound.
No kernel may reach another device: no remote copies, remote signals or barrier semaphores. Data moves between devices by JAX's collectives and lax.ppermute only.
A program may use at most 128 MiB of HBM per device.

```python
import math
import jax
import jax.numpy as jnp
import numpy as np
from jax import lax

EXPERTS = 8
DW = 2048
H = 7168
TOK_DEV = 128
CAP = 48
SLOTS_E = 384
BLOCKS = 32
TOKENS = 4096
N_GRP = 4
N_EP = 8


def draw_live_tokens(key, part):
    index = jnp.arange(BLOCKS, dtype=jnp.int32)
    lowest = TOK_DEV // 4
    base = lowest + (TOK_DEV - lowest) * index // max(BLOCKS - 1, 1)
    jitter = jax.random.randint(jax.random.fold_in(key, 17), (BLOCKS,), 0, TOK_DEV // 8 + 1, dtype=jnp.int32)
    jitter = jnp.where(index == BLOCKS - 1, 0, jitter)
    return jnp.clip(base - jitter, 1, TOK_DEV).astype(jnp.int32)


def block_levels(key, extent, shards, low, top_value):
    def one(dim, blocks):
        draws = jax.random.uniform(jax.random.fold_in(jax.random.fold_in(key, 6), dim), (blocks,), jnp.float32, low / len(shards), top_value / len(shards))
        return jnp.repeat(jnp.exp(draws), extent[dim] // blocks).reshape((-1,) + (1,) * (len(extent) - dim - 1))

    factor_of = one(*shards[0])
    for cut in shards[1:]:
        factor_of = factor_of * one(*cut)
    return factor_of


def assign_block(key, own, number, rows, amount, top, most, skew):
    sequence = jax.random.permutation(key, amount)
    crowded, common = load_shares(amount, rows * top, most, skew, True), load_shares(amount, rows * top, most, skew, False)
    places = jnp.arange(amount)

    def named(sizes, offset_by):
        used = int((sizes > 0).sum())
        fixed = max(1, used // 4)
        moved = fixed + (places - fixed + offset_by * (used - fixed)) % max(1, amount - fixed)
        return jnp.zeros((amount,), jnp.int32).at[sequence[jnp.where(places < fixed, places, moved)]].set(jnp.asarray(sizes, jnp.int32))

    sizes = jnp.where(number % 4 == 0, named(crowded, number // 4), named(common, number - number // 4 - 1))
    mixed = jax.random.permutation(jax.random.fold_in(own, 3), amount)
    donor, taker = mixed[0:amount // 2 * 2:2], mixed[1:amount // 2 * 2:2]
    slack = jnp.minimum(sizes[donor] - 1, most - sizes[taker]) // 2
    slack = jnp.where((donor == sequence[0]) | (taker == sequence[0]) | (sizes[taker] == 0), 0, jnp.maximum(slack, 0))
    moved = jax.random.randint(jax.random.fold_in(own, 4), (amount // 2,), 0, 1 << 20) % (slack + 1)
    sizes = sizes.at[donor].add(-moved).at[taker].add(moved)
    items = jnp.searchsorted(jnp.cumsum(sizes), jnp.arange(rows * top), side="right").astype(jnp.int32)
    table = items.reshape(top, rows).T
    table = table[jax.random.permutation(jax.random.fold_in(own, 1), rows)]
    offset_by = jax.random.randint(jax.random.fold_in(own, 2), (rows, 1), 0, top)
    return jnp.take_along_axis(table, (jnp.arange(top)[None, :] + offset_by) % top, axis=1)


def load_shares(amount, total, bound, skew, full):
    portions = [(1 << 20) // math.isqrt(grade ** skew) + 1 for grade in range(1, amount + 1)]
    largest = bound if full else min(bound, max(-(-total // amount), total * portions[0] // sum(portions)))
    least = 1 if total - largest >= amount - 1 else 0
    given, spare = [largest] + [least] * (amount - 1), total - largest - least * (amount - 1)
    while spare > 0:
        movable = [i for i in range(1, amount) if given[i] < largest] or [i for i in range(1, amount) if given[i] < bound]
        whole, budget = sum([portions[i] for i in movable]), spare
        for i in movable:
            addition = min(bound - given[i], max(1, budget * portions[i] // whole), spare)
            given[i] = given[i] + addition
            spare = spare - addition
    return np.array(given)


def noise(own_key, extent, deviation, limit, shards=(), held_as=jnp.bfloat16):
    gain = block_levels(own_key, extent, shards, -0.22, 0.18) if shards else 1.0
    array = jax.random.normal(own_key, extent, jnp.float32) * deviation * gain
    return jnp.minimum(jnp.maximum(array, -limit), limit).astype(held_as)


def setup_inputs(seed: int = 0) -> dict:
    streams_of = jax.random.split(jax.random.key(seed), 6)
    d_out = noise(streams_of[0], (TOKENS, DW), 2.0, 12.0, ((0, 32),))
    routes_keys = jax.random.split(jax.random.fold_in(streams_of[1], 1), TOKENS // TOK_DEV)
    routes_turns = jax.random.permutation(jax.random.fold_in(streams_of[1], 3), TOKENS // TOK_DEV)
    routes = jax.vmap(lambda own, number: assign_block(jax.random.fold_in(streams_of[1], 2), own, number, TOK_DEV, EXPERTS, 2, CAP, 2))(routes_keys, routes_turns).reshape((TOKENS, 2))
    combine = jnp.clip(jnp.exp(math.log(1.0) - 2.9957323 * jax.random.uniform(streams_of[2], (TOKENS, 2), jnp.float32) ** block_levels(streams_of[2], (TOKENS, 2), ((0, 32),), -0.2, 0.2)), 0.05, 1.0)
    live_tokens = draw_live_tokens(jax.random.fold_in(streams_of[5], 71), 0)
    hidden = noise(streams_of[4], (N_GRP * SLOTS_E, EXPERTS * H), 1.0, 6.0, ((0, 4), (1, 8)))
    return dict(d_out=d_out, routes=routes, combine=combine, live_tokens=live_tokens, hidden=hidden)


def device_slots(d_rows, route_rows, weight_rows, live_count):
    tokens_here = d_rows.shape[0]
    alive = (jnp.arange(tokens_here, dtype=jnp.int32) < live_count).astype(jnp.float32)
    scaled = weight_rows * alive[:, None]
    weighted = (d_rows.astype(jnp.float32)[:, None, :] * scaled[:, :, None]).astype(jnp.bfloat16)
    weighted = weighted.reshape(tokens_here * route_rows.shape[1], d_rows.shape[1])
    flat = route_rows.reshape(-1).astype(jnp.int32)
    chosen = (flat[:, None] == jnp.arange(EXPERTS, dtype=jnp.int32)[None, :]).astype(jnp.int32)
    before = (jnp.cumsum(chosen, axis=0, dtype=jnp.int32) - chosen).astype(jnp.int32)
    position = lax.optimization_barrier(jnp.sum(before * chosen, axis=1, dtype=jnp.int32))
    slot_index = (flat * CAP + position).astype(jnp.int32)
    placing = (jnp.arange(EXPERTS * CAP, dtype=jnp.int32)[:, None] == slot_index[None, :]).astype(jnp.bfloat16)
    buffer = jnp.dot(placing, weighted, preferred_element_type=jnp.float32).astype(jnp.bfloat16)
    alive_pairs = jnp.repeat(alive, route_rows.shape[1])
    counts = lax.optimization_barrier(jnp.sum(chosen.astype(jnp.float32) * alive_pairs[:, None], axis=0))
    return (buffer.reshape(EXPERTS, CAP, d_rows.shape[1]), counts)

def reference(d_out, routes, combine, live_tokens, hidden):
    width = d_out.shape[1]
    group_tokens = N_EP * TOK_DEV

    def group_part(group):
        start = (group * group_tokens).astype(jnp.int32)
        rows = lax.dynamic_slice_in_dim(d_out, start, group_tokens, 0).reshape(N_EP, TOK_DEV, width)
        picks = lax.dynamic_slice_in_dim(routes, start, group_tokens, 0).reshape(N_EP, TOK_DEV, 2)
        weights = lax.dynamic_slice_in_dim(combine, start, group_tokens, 0).reshape(N_EP, TOK_DEV, 2)
        lives = lax.dynamic_slice_in_dim(live_tokens, (group * N_EP).astype(jnp.int32), N_EP, 0)
        buffers, counts = jax.vmap(device_slots)(rows, picks, weights, lives)

        def one_expert(expert):
            slots = lax.dynamic_index_in_dim(buffers, expert, 1, keepdims=False).reshape(N_EP * CAP, width)
            block = lax.dynamic_slice(hidden, ((group * SLOTS_E).astype(jnp.int32), (expert * H).astype(jnp.int32)), (SLOTS_E, H))
            return lax.dot_general(slots, block, (((0,), (0,)), ((), ())), preferred_element_type=jnp.float32)
        partial_value = lax.map(one_expert, jnp.arange(EXPERTS, dtype=jnp.int32))
        return (partial_value, lax.optimization_barrier(jnp.sum(counts, axis=0)))

    def step(carry, group):
        total, count = carry
        partial_value, counts = group_part(group)
        return ((total + partial_value, count + counts), None)
    start = (jnp.zeros((EXPERTS, width, H), jnp.float32), jnp.zeros((EXPERTS,), jnp.float32))
    (total, count), _ = lax.scan(step, start, jnp.arange(N_GRP, dtype=jnp.int32))
    result = total * lax.rsqrt(1.0 + count)[:, None, None]
    return jnp.transpose(result, (1, 0, 2)).reshape(width, EXPERTS * H)
```

```python
import functools

import jax
import jax.numpy as jnp
from jax import lax
from jax.experimental import pallas as pl
from jax.experimental.pallas import tpu as pltpu
from jax.sharding import PartitionSpec as P

EXPERTS = 8
CAP = 48
LANES = 128
CHUNKS = 4


def shift_perm(size, cores, dy, dc):
    chips = size // cores
    return [
        (y * cores + c, ((y + dy) % chips) * cores + (c ^ dc)) for y in range(chips) for c in range(cores)
    ]


def split_count(extent, most):
    units = extent // LANES
    return max(n for n in range(1, most + 1) if units % n == 0)


def token_plan(routes, combine, live_count):
    tokens, top = routes.shape
    alive = (jnp.arange(tokens, dtype=jnp.int32) < live_count).astype(jnp.float32)
    weights = (combine * alive[:, None]).T
    picks = routes.T
    chosen = (picks[:, :, None] == jnp.arange(EXPERTS, dtype=jnp.int32)).astype(jnp.float32)
    named = jnp.sum(chosen, axis=0)
    row = jnp.arange(tokens, dtype=jnp.int32)
    earlier = (row[None, :] < row[:, None]).astype(jnp.bfloat16)
    before = jnp.dot(earlier, named.astype(jnp.bfloat16), preferred_element_type=jnp.float32)
    position = jnp.sum(before[None] * chosen, axis=2)
    slot = picks.astype(jnp.float32) * CAP + position
    counts = jnp.sum(named * alive[:, None], axis=0)
    return jnp.concatenate([slot, weights], axis=0), counts


def place(d_cols, meta):
    top = meta.shape[0] // 2
    slot, weights = meta[:top], meta[top:]
    weighted = (d_cols.astype(jnp.float32)[None] * weights[:, :, None]).astype(jnp.bfloat16)
    weighted = weighted.reshape(-1, d_cols.shape[1])
    placing = (
        jnp.arange(EXPERTS * CAP, dtype=jnp.int32)[:, None] == slot.reshape(-1).astype(jnp.int32)[None, :]
    ).astype(jnp.bfloat16)
    return jnp.dot(placing, weighted, preferred_element_type=jnp.float32).astype(jnp.bfloat16)


def grad_body(pieces, rows, scale_ref, lhs_ref, *refs):
    out_ref = refs[-1]
    acc = None
    for j in range(pieces):
        part = jnp.dot(
            lhs_ref[:, j * rows : (j + 1) * rows], refs[j][...], preferred_element_type=jnp.float32
        )
        acc = part if acc is None else acc + part
    out_ref[...] = acc * scale_ref[0, 0]


def grad_chunk(scale, lhs, own, others, chunk, chunk_cols, out):
    rows, total_cols = own.shape
    width, depth = lhs.shape
    pieces = 1 + len(others)
    units = chunk_cols // LANES
    fits = [
        n
        for n in range(1, units + 1)
        if units % n == 0 and n * LANES * (4 * depth + 8 * width) <= 16 * 2**20
    ]
    block = max(fits + [1]) * LANES
    steps = chunk_cols // block
    base = chunk * steps
    in_specs = [
        pl.BlockSpec(memory_space=pltpu.SMEM),
        pl.BlockSpec((width, depth), lambda i: (0, 0)),
        pl.BlockSpec((rows, block), lambda i: (0, base + i)),
    ] + [pl.BlockSpec((rows, block), lambda i: (0, i)) for _ in others]
    operands = [scale, lhs, own, *others]
    aliases = {}
    if out is not None:
        in_specs.append(pl.BlockSpec(memory_space=pl.ANY))
        aliases = {len(operands): 0}
        operands.append(out)
    return pl.pallas_call(
        functools.partial(grad_body, pieces, rows),
        grid=(steps,),
        in_specs=in_specs,
        out_specs=pl.BlockSpec((width, block), lambda i: (0, base + i)),
        out_shape=jax.ShapeDtypeStruct((width, total_cols), jnp.float32),
        input_output_aliases=aliases,
        compiler_params=pltpu.CompilerParams(
            dimension_semantics=("arbitrary",), vmem_limit_bytes=48 * 2**20
        ),
    )(*operands)


def on_device(d_out, routes, combine, live_tokens, hidden):
    groups = lax.axis_size("grp")
    cores = 2 if groups % 2 == 0 else 1
    chips = groups // cores
    ranks = lax.axis_size("ep")
    shards = ranks // EXPERTS
    my_expert = lax.axis_index("ep") // shards
    me = lax.axis_index("grp")
    my_chip, my_core = me // cores, me % cores
    block = d_out.shape[1] // groups

    meta, counts = token_plan(routes, combine, live_tokens[0])
    offsets = [(dy, dc) for dy in range(chips) for dc in range(cores)]
    tokens, metas = [], []
    for dy, dc in offsets:
        target = ((my_chip + dy) % chips) * cores + (my_core ^ dc)
        cols = lax.dynamic_slice_in_dim(d_out, target * block, block, 1)
        if (dy, dc) == (0, 0):
            tokens.append(cols)
            metas.append(meta)
            continue
        perm = shift_perm(groups, cores, dy, dc)
        tokens.append(lax.ppermute(cols, "grp", perm))
        metas.append(lax.ppermute(meta, "grp", perm))

    n_chunks = split_count(hidden.shape[1], CHUNKS)
    chunk_cols = hidden.shape[1] // n_chunks
    pieces = []
    for c in range(n_chunks):
        mine = hidden[:, c * chunk_cols : (c + 1) * chunk_cols]
        got = []
        for dy in range(chips):
            here = mine if dy == 0 else lax.ppermute(mine, "grp", shift_perm(groups, cores, dy, 0))
            if dy > 0:
                got.append(here)
            if cores > 1:
                got.append(lax.ppermute(here, "grp", shift_perm(groups, cores, 0, 1)))
        pieces.append(got)

    placed = jnp.stack(
        [place(t, m).reshape(EXPERTS, CAP, block) for t, m in zip(tokens, metas)], axis=1
    )
    sending = jnp.repeat(placed, shards, axis=0)
    arrived = lax.all_to_all(sending, "ep", split_axis=0, concat_axis=0, tiled=True)
    lhs = jnp.transpose(arrived, (3, 1, 0, 2)).reshape(block, groups * ranks * CAP)

    totals = lax.psum(counts, ("grp", "ep"))
    picked = (jnp.arange(EXPERTS, dtype=jnp.int32) == my_expert).astype(jnp.float32)
    scale = lax.rsqrt(1.0 + jnp.sum(totals * picked)).reshape(1, 1)

    out = None
    for c in range(n_chunks):
        out = grad_chunk(scale, lhs, hidden, pieces[c], c, chunk_cols, out)
    return out


def solution(mesh):
    return jax.shard_map(
        on_device,
        mesh=mesh,
        in_specs=(
            P(("grp", "ep"), None),
            P(("grp", "ep"), None),
            P(("grp", "ep"), None),
            P(("grp", "ep")),
            P("grp", "ep"),
        ),
        out_specs=P("grp", "ep"),
        check_vma=False,
    )
```
